32 devices in a mesh: vocab: 8 (over z, y), batch: 4 (over x, core).
Axes of the slice: x: 2, y: 2, z: 4, core: 2. Of those that a mesh axis runs over, the one named last changes fastest.
Arguments:
- latent_vectors: bfloat16 [2048, 4608], P(('batch', 'vocab')), parts along dimension 0, may hold values from -8 to 8
- unembedding_matrix: bfloat16 [18432, 8192], P('batch', 'vocab'), parts along dimension 0, may hold values from -1 to 1
- sampler_heat: float32 [2048], P('batch'), parts along dimension 0, may hold values from 0.1 to 1
Outputs:
- probs: bfloat16 [2048, 8192], P(('batch', 'vocab')), parts along dimension 0
- lse: float32 [2048], P(('batch', 'vocab')), parts along dimension 0
- z_loss: float32 [2048], P(('batch', 'vocab')), parts along dimension 0
The draws below stay inside these ranges and needn't reach their ends.
There are 4 independent parts, one for each index of `batch`. The reference program is written for one: setup_inputs(seed, part) draws one part's arguments, and reference() takes and returns one part's arrays. A program takes and returns all parts, laid end to end along the dimension named above; each array names one. Nothing has to cross between parts.
All inputs are finite; a program needn't handle non-finite values.
Results may differ from the reference program's by a relative error of at most 0.00115.
Values may be sent and summed in bfloat16 or wider, within the bound.
A program may use at most 64 MiB of HBM per device.

```python
import math
import jax
import jax.numpy as jnp

D = 4608
PROMPT_NUMBER = 512
VOCAB = 8192


def vocab_weight(key):
    gaussian_draw = jax.random.normal(jax.random.fold_in(key, 11), (D, VOCAB), jnp.float32)
    return jnp.clip(gaussian_draw, -4.0, 4.0) / math.sqrt(D)


def draw_unembedding_matrix(key, part):
    return vocab_weight(key).astype(jnp.bfloat16)


def draw_latent_vectors(key, part):
    hidden_states = jnp.clip(jax.random.normal(jax.random.fold_in(key, 23), (PROMPT_NUMBER, D), jnp.float32), -6.0, 6.0)
    return hidden_states.astype(jnp.bfloat16)


def draw_sampler_heat(key, part):
    heat = jax.random.uniform(jax.random.fold_in(key, 41), (PROMPT_NUMBER,), jnp.float32, 0.8, 1.0)
    return heat.astype(jnp.float32)


def setup_inputs(seed: int = 0, part: int = 0) -> dict:
    splits = jax.random.split(jax.random.key(seed), 4)
    part_splits = jax.random.split(jax.random.fold_in(splits[3], part), 4)
    return {
        "latent_vectors": draw_latent_vectors(jax.random.fold_in(jax.random.fold_in(splits[3], part), 71), part),
        "unembedding_matrix": draw_unembedding_matrix(jax.random.fold_in(jax.random.fold_in(splits[3], part), 71), part),
        "sampler_heat": draw_sampler_heat(jax.random.fold_in(jax.random.fold_in(splits[3], part), 71), part),
    }


def reference(latent_vectors, unembedding_matrix, sampler_heat):
    logits = jnp.dot(latent_vectors, unembedding_matrix, preferred_element_type=jnp.float32)
    bounded_scores = 30.0 * jnp.tanh(logits / 30.0)
    heat_scaled_scores = bounded_scores / sampler_heat[:, None]
    peak = jnp.max(heat_scaled_scores, axis=1)
    total = jnp.sum(jnp.exp(heat_scaled_scores - peak[:, None]), axis=1)
    lse = peak + jnp.log(total)
    z_loss = 0.0001 * lse * lse
    probs = jnp.exp(heat_scaled_scores - lse[:, None]).astype(jnp.bfloat16)
    return probs, lse, z_loss
```

```python
import functools

import jax
import jax.numpy as jnp
from jax import lax
from jax.experimental import pallas as pl
from jax.experimental.pallas import tpu as pltpu
from jax.sharding import PartitionSpec as P

MESH = pl.DeviceIdType.MESH
UP, DOWN, SIDE = 0, 1, 2


def each(count, body):
    if count <= 8:
        for k in range(count):
            body(k)
    else:
        lax.fori_loop(0, count, lambda k, c: (body(k), c)[1], 0)


def kernel(n, waves, x_ref, w_hbm, heat_ref, probs_ref, lse_ref, w_ref, buf, scaled, outbox, stats, lse_col,
           w_sem, own_sem, ag_send, ag_recv, st_send, st_recv, pr_send, pr_recv):
    me = lax.axis_index("vocab")
    line = n // 2
    z, y = me // 2, lax.rem(me, 2)
    seq = x_ref.shape[0]
    rows = seq // waves
    span = n * rows
    cols = w_ref.shape[1]
    tile = min(cols, 256)

    barrier = pltpu.get_barrier_semaphore()

    def greet(k):
        pl.semaphore_signal(barrier, inc=1, device_id={"vocab": lax.rem(me + k + 1, n)}, device_id_type=MESH)

    each(n - 1, greet)
    weights = pltpu.make_async_copy(w_hbm, w_ref, w_sem)
    weights.start()
    for w in range(waves):
        pltpu.make_async_copy(x_ref.at[pl.ds(w * rows, rows)], buf.at[w, me], own_sem.at[w]).start()
    for w in range(waves):
        pltpu.make_async_copy(x_ref.at[pl.ds(w * rows, rows)], buf.at[w, me], own_sem.at[w]).wait()
    pl.semaphore_wait(barrier, n - 1)

    def hop(w, block, way):
        target = {UP: lax.rem(me + 2, n), DOWN: lax.rem(me + n - 2, n), SIDE: me + 1 - 2 * y}[way]
        return pltpu.make_async_remote_copy(
            src_ref=buf.at[w, block], dst_ref=buf.at[w, block], send_sem=ag_send.at[w, block, way],
            recv_sem=ag_recv.at[w, block], device_id={"vocab": target}, device_id_type=MESH)

    def send_own(w):
        @pl.when(z < line - 1)
        def _():
            hop(w, me, UP).start()

        @pl.when(z > 0)
        def _():
            hop(w, me, DOWN).start()

        hop(w, me, SIDE).start()

    def relay(w, k):
        @pl.when(z >= k)
        def _():
            block = (z - k) * 2 + y
            hop(w, block, SIDE).wait_recv()

            @pl.when(z < line - 1)
            def _():
                hop(w, block, UP).start()

            hop(w, block, SIDE).start()

        @pl.when(z + k < line)
        def _():
            block = (z + k) * 2 + y
            hop(w, block, SIDE).wait_recv()

            @pl.when(z > 0)
            def _():
                hop(w, block, DOWN).start()

            hop(w, block, SIDE).start()

    def stat_copy(w, k):
        return pltpu.make_async_remote_copy(
            src_ref=stats.at[w, me], dst_ref=stats.at[w, me], send_sem=st_send.at[w, k],
            recv_sem=st_recv.at[w, me], device_id={"vocab": lax.rem(me + k + 1, n)}, device_id_type=MESH)

    def stat_wait(w, k):
        other = lax.rem(me + k + 1, n)
        pltpu.make_async_remote_copy(
            src_ref=stats.at[w, other], dst_ref=stats.at[w, other], send_sem=st_send.at[w, k],
            recv_sem=st_recv.at[w, other], device_id={"vocab": other}, device_id_type=MESH).wait_recv()

    def out_at(w, owner):
        return probs_ref.at[pl.ds(w * rows, rows), pl.ds(pl.multiple_of(owner * cols, cols), cols)]

    def prob_copy(w, k):
        other = lax.rem(me + k + 1, n)
        return pltpu.make_async_remote_copy(
            src_ref=outbox.at[w, other], dst_ref=out_at(w, me), send_sem=pr_send.at[w, k],
            recv_sem=pr_recv.at[w, me], device_id={"vocab": other}, device_id_type=MESH)

    def prob_wait(w, k):
        other = lax.rem(me + k + 1, n)
        pltpu.make_async_remote_copy(
            src_ref=outbox.at[w, other], dst_ref=out_at(w, other), send_sem=pr_send.at[w, k],
            recv_sem=pr_recv.at[w, other], device_id={"vocab": other}, device_id_type=MESH).wait_recv()

    def score(w):
        def arrive(k):
            hop(w, k * 2 + 1 - y, SIDE).wait_recv()

        each(line, arrive)
        if w == 0:
            weights.wait()
        hidden = buf[w].reshape(span, buf.shape[3])
        cool = 1.0 / jnp.broadcast_to(heat_ref[w], (8, span)).T[:, :1]

        def column(j, peak):
            at = pl.ds(pl.multiple_of(j * tile, tile), tile)
            logits = jnp.dot(hidden, w_ref[:, at], preferred_element_type=jnp.float32)
            s = 30.0 * jnp.tanh(logits * (1.0 / 30.0)) * cool
            scaled[:, at] = s
            return jnp.maximum(peak, jnp.max(s, axis=1, keepdims=True))

        peak = lax.fori_loop(0, cols // tile, column, jnp.full((span, 1), -jnp.inf, jnp.float32))
        total = jnp.sum(jnp.exp(scaled[...] - peak), axis=1, keepdims=True)
        lane = lax.broadcasted_iota(jnp.int32, (span, 128), 1)
        stats[w, me] = jnp.where(lane == 0, peak, total).T[:8]
        each(n - 1, lambda k: stat_copy(w, k).start())

    def finish(w):
        each(n - 1, lambda k: stat_wait(w, k))
        got = stats[w]
        peaks, totals = got[:, 0, :], got[:, 1, :]
        peak = jnp.max(peaks, axis=0, keepdims=True)
        lse = peak + jnp.log(jnp.sum(totals * jnp.exp(peaks - peak), axis=0, keepdims=True))
        lse = jnp.broadcast_to(lse, (8, span)).T[:, :1]
        probs = jnp.exp(scaled[...] - lse).astype(jnp.bfloat16)
        outbox[w] = probs.reshape(n, rows, cols)
        each(n - 1, lambda k: prob_copy(w, k).start())
        lse_col[...] = jnp.broadcast_to(lse, (span, 128)).reshape(n, rows, 128)
        lse_ref[pl.ds(w * rows, rows), :] = lse_col[me]
        probs_ref[pl.ds(w * rows, rows), pl.ds(pl.multiple_of(me * cols, cols), cols)] = outbox[w, me]

    send_own(0)
    for w in range(waves):
        todo = []
        if w >= 1:
            todo = [functools.partial(score, w - 1), functools.partial(finish, w - 1)]
        if line - 1 <= 8:
            for k in range(1, line):
                relay(w, k)
                if k == 1 and w + 1 < waves:
                    send_own(w + 1)
                if todo:
                    todo.pop(0)()
        else:
            if w + 1 < waves:
                send_own(w + 1)
            each(line - 1, lambda k: relay(w, k + 1))
        while todo:
            todo.pop(0)()
    score(waves - 1)
    finish(waves - 1)

    for w in range(waves):
        each(n - 1, lambda k: prob_wait(w, k))

        def drain(k):
            block = k * 2 + y

            @pl.when(jnp.logical_and(z < line - 1, k <= z))
            def _():
                hop(w, block, UP).wait_send()

            @pl.when(jnp.logical_and(z > 0, k >= z))
            def _():
                hop(w, block, DOWN).wait_send()

            hop(w, block, SIDE).wait_send()

        each(line, drain)
        each(n - 1, lambda k: stat_copy(w, k).wait_send())
        each(n - 1, lambda k: prob_copy(w, k).wait_send())


def solution(mesh):
    n = mesh.shape["vocab"]

    def local(latent_vectors, unembedding_matrix, sampler_heat):
        seq, depth = latent_vectors.shape
        cols = unembedding_matrix.shape[1]
        waves = max(1, seq // 32)
        rows = seq // waves
        span = n * rows
        heat = sampler_heat.reshape(n, waves, rows).transpose(1, 0, 2).reshape(waves, 1, span)
        vmem = pl.BlockSpec(memory_space=pltpu.VMEM)
        dma = pltpu.SemaphoreType.DMA
        probs, lse = pl.pallas_call(
            functools.partial(kernel, n, waves),
            out_shape=(jax.ShapeDtypeStruct((seq, n * cols), jnp.bfloat16),
                       jax.ShapeDtypeStruct((seq, 128), jnp.float32)),
            in_specs=[vmem, pl.BlockSpec(memory_space=pl.ANY), vmem],
            out_specs=(vmem, vmem),
            scratch_shapes=[
                pltpu.VMEM((depth, cols), jnp.bfloat16),
                pltpu.VMEM((waves, n, rows, depth), jnp.bfloat16),
                pltpu.VMEM((span, cols), jnp.float32),
                pltpu.VMEM((waves, n, rows, cols), jnp.bfloat16),
                pltpu.VMEM((waves, n, 8, span), jnp.float32),
                pltpu.VMEM((n, rows, 128), jnp.float32),
                dma, dma((waves,)),
                dma((waves, n, 3)), dma((waves, n)),
                dma((waves, n - 1)), dma((waves, n)),
                dma((waves, n - 1)), dma((waves, n)),
            ],
            compiler_params=pltpu.CompilerParams(
                collective_id=0, has_side_effects=True, vmem_limit_bytes=56 * 1024 * 1024),
        )(latent_vectors, unembedding_matrix, heat)
        lse = lse[:, 0]
        return probs, lse, 0.0001 * lse * lse

    in_specs = (P(("batch", "vocab"), None), P("batch", "vocab"), P("batch"))
    out_specs = (P(("batch", "vocab"), None), P(("batch", "vocab")), P(("batch", "vocab")))
    return jax.shard_map(local, mesh=mesh, in_specs=in_specs, out_specs=out_specs, check_vma=False)
```

```python
import functools

import jax
import jax.numpy as jnp
from jax import lax
from jax.experimental import pallas as pl
from jax.experimental.pallas import tpu as pltpu
from jax.sharding import PartitionSpec as P

MESH = pl.DeviceIdType.MESH
UP, DOWN, SIDE = 0, 1, 2


def each(count, body):
    if count <= 8:
        for k in range(count):
            body(k)
    else:
        lax.fori_loop(0, count, lambda k, c: (body(k), c)[1], 0)


def kernel(n, waves, x_ref, w_hbm, heat_ref, probs_ref, lse_ref, w_ref, buf, scaled, outbox, stats, lse_col,
           w_sem, own_sem, ag_send, ag_recv, st_send, st_recv, pr_send, pr_recv):
    me = lax.axis_index("vocab")
    line = n // 2
    z, y = me // 2, lax.rem(me, 2)
    seq = x_ref.shape[0]
    rows = seq // waves
    span = n * rows
    cols = w_ref.shape[1]
    tile = min(cols, 256)

    barrier = pltpu.get_barrier_semaphore()

    def greet(k):
        pl.semaphore_signal(barrier, inc=1, device_id={"vocab": lax.rem(me + k + 1, n)}, device_id_type=MESH)

    each(n - 1, greet)
    weights = pltpu.make_async_copy(w_hbm, w_ref, w_sem)
    weights.start()
    for w in range(waves):
        pltpu.make_async_copy(x_ref.at[pl.ds(w * rows, rows)], buf.at[w, me], own_sem.at[w]).start()
    for w in range(waves):
        pltpu.make_async_copy(x_ref.at[pl.ds(w * rows, rows)], buf.at[w, me], own_sem.at[w]).wait()
    pl.semaphore_wait(barrier, n - 1)

    def hop(w, block, way):
        target = {UP: lax.rem(me + 2, n), DOWN: lax.rem(me + n - 2, n), SIDE: me + 1 - 2 * y}[way]
        return pltpu.make_async_remote_copy(
            src_ref=buf.at[w, block], dst_ref=buf.at[w, block], send_sem=ag_send.at[w, block, way],
            recv_sem=ag_recv.at[w, block], device_id={"vocab": target}, device_id_type=MESH)

    def send_own(w):
        @pl.when(z < line - 1)
        def _():
            hop(w, me, UP).start()

        @pl.when(z > 0)
        def _():
            hop(w, me, DOWN).start()

        hop(w, me, SIDE).start()

    def relay(w, k):
        @pl.when(z >= k)
        def _():
            block = (z - k) * 2 + y
            hop(w, block, SIDE).wait_recv()

            @pl.when(z < line - 1)
            def _():
                hop(w, block, UP).start()

            hop(w, block, SIDE).start()

        @pl.when(z + k < line)
        def _():
            block = (z + k) * 2 + y
            hop(w, block, SIDE).wait_recv()

            @pl.when(z > 0)
            def _():
                hop(w, block, DOWN).start()

            hop(w, block, SIDE).start()

    def stat_copy(w, k):
        return pltpu.make_async_remote_copy(
            src_ref=stats.at[w, me], dst_ref=stats.at[w, me], send_sem=st_send.at[w, k],
            recv_sem=st_recv.at[w, me], device_id={"vocab": lax.rem(me + k + 1, n)}, device_id_type=MESH)

    def stat_wait(w, k):
        other = lax.rem(me + k + 1, n)
        pltpu.make_async_remote_copy(
            src_ref=stats.at[w, other], dst_ref=stats.at[w, other], send_sem=st_send.at[w, k],
            recv_sem=st_recv.at[w, other], device_id={"vocab": other}, device_id_type=MESH).wait_recv()

    def out_at(w, owner):
        return probs_ref.at[pl.ds(w * rows, rows), pl.ds(pl.multiple_of(owner * cols, cols), cols)]

    def prob_copy(w, k):
        other = lax.rem(me + k + 1, n)
        return pltpu.make_async_remote_copy(
            src_ref=outbox.at[w, other], dst_ref=out_at(w, me), send_sem=pr_send.at[w, k],
            recv_sem=pr_recv.at[w, me], device_id={"vocab": other}, device_id_type=MESH)

    def prob_wait(w, k):
        other = lax.rem(me + k + 1, n)
        pltpu.make_async_remote_copy(
            src_ref=outbox.at[w, other], dst_ref=out_at(w, other), send_sem=pr_send.at[w, k],
            recv_sem=pr_recv.at[w, other], device_id={"vocab": other}, device_id_type=MESH).wait_recv()

    def score(w):
        def arrive(k):
            hop(w, k * 2 + 1 - y, SIDE).wait_recv()

        each(line, arrive)
        if w == 0:
            weights.wait()
        hidden = buf[w].reshape(span, buf.shape[3])
        cool = 1.0 / jnp.broadcast_to(heat_ref[w], (8, span)).T[:, :1]

        def column(j, peak):
            at = pl.ds(pl.multiple_of(j * tile, tile), tile)
            logits = jnp.dot(hidden, w_ref[:, at], preferred_element_type=jnp.float32)
            s = 30.0 * jnp.tanh(logits * (1.0 / 30.0)) * cool
            scaled[:, at] = s
            return jnp.maximum(peak, jnp.max(s, axis=1, keepdims=True))

        peak = lax.fori_loop(0, cols // tile, column, jnp.full((span, 1), -jnp.inf, jnp.float32))
        total = jnp.sum(jnp.exp(scaled[...] - peak), axis=1, keepdims=True)
        lane = lax.broadcasted_iota(jnp.int32, (span, 128), 1)
        stats[w, me] = jnp.where(lane == 0, peak, total).T[:8]
        each(n - 1, lambda k: stat_copy(w, k).start())

    def finish(w):
        each(n - 1, lambda k: stat_wait(w, k))
        got = stats[w]
        peaks, totals = got[:, 0, :], got[:, 1, :]
        peak = jnp.max(peaks, axis=0, keepdims=True)
        lse = peak + jnp.log(jnp.sum(totals * jnp.exp(peaks - peak), axis=0, keepdims=True))
        lse = jnp.broadcast_to(lse, (8, span)).T[:, :1]
        probs = jnp.exp(scaled[...] - lse).astype(jnp.bfloat16)
        outbox[w] = probs.reshape(n, rows, cols)
        each(n - 1, lambda k: prob_copy(w, k).start())
        lse_col[...] = jnp.broadcast_to(lse, (span, 128)).reshape(n, rows, 128)
        lse_ref[pl.ds(w * rows, rows), :] = lse_col[me]
        probs_ref[pl.ds(w * rows, rows), pl.ds(pl.multiple_of(me * cols, cols), cols)] = outbox[w, me]

    send_own(0)
    for w in range(waves):
        todo = []
        if w >= 1:
            todo = [functools.partial(score, w - 1), functools.partial(finish, w - 1)]
        if line - 1 <= 8:
            for k in range(1, line):
                relay(w, k)
                if k == 1 and w + 1 < waves:
                    send_own(w + 1)
                if todo and k >= 2:
                    todo.pop(0)()
        else:
            if w + 1 < waves:
                send_own(w + 1)
            each(line - 1, lambda k: relay(w, k + 1))
        while todo:
            todo.pop(0)()
    score(waves - 1)
    finish(waves - 1)

    for w in range(waves):
        each(n - 1, lambda k: prob_wait(w, k))

        def drain(k):
            block = k * 2 + y

            @pl.when(jnp.logical_and(z < line - 1, k <= z))
            def _():
                hop(w, block, UP).wait_send()

            @pl.when(jnp.logical_and(z > 0, k >= z))
            def _():
                hop(w, block, DOWN).wait_send()

            hop(w, block, SIDE).wait_send()

        each(line, drain)
        each(n - 1, lambda k: stat_copy(w, k).wait_send())
        each(n - 1, lambda k: prob_copy(w, k).wait_send())


def solution(mesh):
    n = mesh.shape["vocab"]

    def local(latent_vectors, unembedding_matrix, sampler_heat):
        seq, depth = latent_vectors.shape
        cols = unembedding_matrix.shape[1]
        waves = max(1, seq // 16)
        rows = seq // waves
        span = n * rows
        heat = sampler_heat.reshape(n, waves, rows).transpose(1, 0, 2).reshape(waves, 1, span)
        vmem = pl.BlockSpec(memory_space=pltpu.VMEM)
        dma = pltpu.SemaphoreType.DMA
        probs, lse = pl.pallas_call(
            functools.partial(kernel, n, waves),
            out_shape=(jax.ShapeDtypeStruct((seq, n * cols), jnp.bfloat16),
                       jax.ShapeDtypeStruct((seq, 128), jnp.float32)),
            in_specs=[vmem, pl.BlockSpec(memory_space=pl.ANY), vmem],
            out_specs=(vmem, vmem),
            scratch_shapes=[
                pltpu.VMEM((depth, cols), jnp.bfloat16),
                pltpu.VMEM((waves, n, rows, depth), jnp.bfloat16),
                pltpu.VMEM((span, cols), jnp.float32),
                pltpu.VMEM((waves, n, rows, cols), jnp.bfloat16),
                pltpu.VMEM((waves, n, 8, span), jnp.float32),
                pltpu.VMEM((n, rows, 128), jnp.float32),
                dma, dma((waves,)),
                dma((waves, n, 3)), dma((waves, n)),
                dma((waves, n - 1)), dma((waves, n)),
                dma((waves, n - 1)), dma((waves, n)),
            ],
            compiler_params=pltpu.CompilerParams(
                collective_id=0, has_side_effects=True, vmem_limit_bytes=56 * 1024 * 1024),
        )(latent_vectors, unembedding_matrix, heat)
        lse = lse[:, 0]
        return probs, lse, 0.0001 * lse * lse

    in_specs = (P(("batch", "vocab"), None), P("batch", "vocab"), P("batch"))
    out_specs = (P(("batch", "vocab"), None), P(("batch", "vocab")), P(("batch", "vocab")))
    return jax.shard_map(local, mesh=mesh, in_specs=in_specs, out_specs=out_specs, check_vma=False)
```

```python
import functools

import jax
import jax.numpy as jnp
from jax import lax
from jax.experimental import pallas as pl
from jax.experimental.pallas import tpu as pltpu
from jax.sharding import PartitionSpec as P

MESH = pl.DeviceIdType.MESH
UP, DOWN, SIDE = 0, 1, 2


def each(count, body):
    if count <= 8:
        for k in range(count):
            body(k)
    else:
        lax.fori_loop(0, count, lambda k, c: (body(k), c)[1], 0)


def kernel(n, waves, x_ref, w_hbm, heat_ref, probs_ref, lse_ref, w_ref, buf, scaled, outbox, stats, lse_col,
           w_sem, own_sem, ag_send, ag_recv, st_send, st_recv, pr_send, pr_recv):
    me = lax.axis_index("vocab")
    line = n // 2
    z, y = me // 2, lax.rem(me, 2)
    seq = x_ref.shape[0]
    rows = seq // waves
    span = n * rows
    cols = w_ref.shape[1]
    tile = min(cols, 256)

    barrier = pltpu.get_barrier_semaphore()

    def greet(k):
        pl.semaphore_signal(barrier, inc=1, device_id={"vocab": lax.rem(me + k + 1, n)}, device_id_type=MESH)

    each(n - 1, greet)
    weights = pltpu.make_async_copy(w_hbm, w_ref, w_sem)
    weights.start()
    for w in range(waves):
        pltpu.make_async_copy(x_ref.at[pl.ds(w * rows, rows)], buf.at[w, me], own_sem.at[w]).start()
    for w in range(waves):
        pltpu.make_async_copy(x_ref.at[pl.ds(w * rows, rows)], buf.at[w, me], own_sem.at[w]).wait()
    pl.semaphore_wait(barrier, n - 1)

    def hop(w, block, way):
        target = {UP: lax.rem(me + 2, n), DOWN: lax.rem(me + n - 2, n), SIDE: me + 1 - 2 * y}[way]
        return pltpu.make_async_remote_copy(
            src_ref=buf.at[w, block], dst_ref=buf.at[w, block], send_sem=ag_send.at[w, block, way],
            recv_sem=ag_recv.at[w, block], device_id={"vocab": target}, device_id_type=MESH)

    def send_own(w):
        @pl.when(z < line - 1)
        def _():
            hop(w, me, UP).start()

        @pl.when(z > 0)
        def _():
            hop(w, me, DOWN).start()

        hop(w, me, SIDE).start()

    def relay(w, k):
        @pl.when(z >= k)
        def _():
            block = (z - k) * 2 + y
            hop(w, block, SIDE).wait_recv()

            @pl.when(z < line - 1)
            def _():
                hop(w, block, UP).start()

            hop(w, block, SIDE).start()

        @pl.when(z + k < line)
        def _():
            block = (z + k) * 2 + y
            hop(w, block, SIDE).wait_recv()

            @pl.when(z > 0)
            def _():
                hop(w, block, DOWN).start()

            hop(w, block, SIDE).start()

    def stat_copy(w, k):
        return pltpu.make_async_remote_copy(
            src_ref=stats.at[w, me], dst_ref=stats.at[w, me], send_sem=st_send.at[w, k],
            recv_sem=st_recv.at[w, me], device_id={"vocab": lax.rem(me + k + 1, n)}, device_id_type=MESH)

    def stat_wait(w, k):
        other = lax.rem(me + k + 1, n)
        pltpu.make_async_remote_copy(
            src_ref=stats.at[w, other], dst_ref=stats.at[w, other], send_sem=st_send.at[w, k],
            recv_sem=st_recv.at[w, other], device_id={"vocab": other}, device_id_type=MESH).wait_recv()

    def out_at(w, owner):
        return probs_ref.at[pl.ds(w * rows, rows), pl.ds(pl.multiple_of(owner * cols, cols), cols)]

    def prob_copy(w, k):
        other = lax.rem(me + k + 1, n)
        return pltpu.make_async_remote_copy(
            src_ref=outbox.at[w, other], dst_ref=out_at(w, me), send_sem=pr_send.at[w, k],
            recv_sem=pr_recv.at[w, me], device_id={"vocab": other}, device_id_type=MESH)

    def prob_wait(w, k):
        other = lax.rem(me + k + 1, n)
        pltpu.make_async_remote_copy(
            src_ref=outbox.at[w, other], dst_ref=out_at(w, other), send_sem=pr_send.at[w, k],
            recv_sem=pr_recv.at[w, other], device_id={"vocab": other}, device_id_type=MESH).wait_recv()

    def score(w):
        def arrive(k):
            hop(w, k * 2 + 1 - y, SIDE).wait_recv()

        each(line, arrive)
        if w == 0:
            weights.wait()
        hidden = buf[w].reshape(span, buf.shape[3])
        cool = 1.0 / jnp.broadcast_to(heat_ref[w], (8, span)).T[:, :1]

        def column(j, peak):
            at = pl.ds(pl.multiple_of(j * tile, tile), tile)
            logits = jnp.dot(hidden, w_ref[:, at], preferred_element_type=jnp.float32)
            s = 30.0 * jnp.tanh(logits * (1.0 / 30.0)) * cool
            scaled[:, at] = s
            return jnp.maximum(peak, jnp.max(s, axis=1, keepdims=True))

        peak = lax.fori_loop(0, cols // tile, column, jnp.full((span, 1), -jnp.inf, jnp.float32))
        total = jnp.sum(jnp.exp(scaled[...] - peak), axis=1, keepdims=True)
        lane = lax.broadcasted_iota(jnp.int32, (span, 128), 1)
        stats[w, me] = jnp.where(lane == 0, peak, total).T[:8]
        each(n - 1, lambda k: stat_copy(w, k).start())

    def finish(w):
        each(n - 1, lambda k: stat_wait(w, k))
        got = stats[w]
        peaks, totals = got[:, 0, :], got[:, 1, :]
        peak = jnp.max(peaks, axis=0, keepdims=True)
        lse = peak + jnp.log(jnp.sum(totals * jnp.exp(peaks - peak), axis=0, keepdims=True))
        lse = jnp.broadcast_to(lse, (8, span)).T[:, :1]
        probs = jnp.exp(scaled[...] - lse).astype(jnp.bfloat16)
        outbox[w] = probs.reshape(n, rows, cols)
        each(n - 1, lambda k: prob_copy(w, k).start())
        lse_col[...] = jnp.broadcast_to(lse, (span, 128)).reshape(n, rows, 128)
        lse_ref[pl.ds(w * rows, rows), :] = lse_col[me]
        probs_ref[pl.ds(w * rows, rows), pl.ds(pl.multiple_of(me * cols, cols), cols)] = outbox[w, me]

    send_own(0)
    for w in range(waves):
        todo = []
        if w >= 1:
            todo = [functools.partial(score, w - 1), functools.partial(finish, w - 1)]
        if line - 1 <= 8:
            for k in range(1, line):
                relay(w, k)
                if k == 1 and w + 1 < waves:
                    send_own(w + 1)
                if todo and k >= 2:
                    todo.pop(0)()
        else:
            if w + 1 < waves:
                send_own(w + 1)
            each(line - 1, lambda k: relay(w, k + 1))
        while todo:
            todo.pop(0)()
    score(waves - 1)
    finish(waves - 1)

    for w in range(waves):
        each(n - 1, lambda k: prob_wait(w, k))

        def drain(k):
            block = k * 2 + y

            @pl.when(jnp.logical_and(z < line - 1, k <= z))
            def _():
                hop(w, block, UP).wait_send()

            @pl.when(jnp.logical_and(z > 0, k >= z))
            def _():
                hop(w, block, DOWN).wait_send()

            hop(w, block, SIDE).wait_send()

        each(line, drain)
        each(n - 1, lambda k: stat_copy(w, k).wait_send())
        each(n - 1, lambda k: prob_copy(w, k).wait_send())


def solution(mesh):
    n = mesh.shape["vocab"]

    def local(latent_vectors, unembedding_matrix, sampler_heat):
        seq, depth = latent_vectors.shape
        cols = unembedding_matrix.shape[1]
        waves = max(1, seq // 32)
        rows = seq // waves
        span = n * rows
        heat = sampler_heat.reshape(n, waves, rows).transpose(1, 0, 2).reshape(waves, 1, span)
        vmem = pl.BlockSpec(memory_space=pltpu.VMEM)
        dma = pltpu.SemaphoreType.DMA
        probs, lse = pl.pallas_call(
            functools.partial(kernel, n, waves),
            out_shape=(jax.ShapeDtypeStruct((seq, n * cols), jnp.bfloat16),
                       jax.ShapeDtypeStruct((seq, 128), jnp.float32)),
            in_specs=[vmem, pl.BlockSpec(memory_space=pl.ANY), vmem],
            out_specs=(vmem, vmem),
            scratch_shapes=[
                pltpu.VMEM((depth, cols), jnp.bfloat16),
                pltpu.VMEM((waves, n, rows, depth), jnp.bfloat16),
                pltpu.VMEM((span, cols), jnp.float32),
                pltpu.VMEM((waves, n, rows, cols), jnp.bfloat16),
                pltpu.VMEM((waves, n, 8, span), jnp.float32),
                pltpu.VMEM((n, rows, 128), jnp.float32),
                dma, dma((waves,)),
                dma((waves, n, 3)), dma((waves, n)),
                dma((waves, n - 1)), dma((waves, n)),
                dma((waves, n - 1)), dma((waves, n)),
            ],
            compiler_params=pltpu.CompilerParams(
                collective_id=0, has_side_effects=True, vmem_limit_bytes=56 * 1024 * 1024),
        )(latent_vectors, unembedding_matrix, heat)
        lse = lse[:, 0]
        return probs, lse, 0.0001 * lse * lse

    in_specs = (P(("batch", "vocab"), None), P("batch", "vocab"), P("batch"))
    out_specs = (P(("batch", "vocab"), None), P(("batch", "vocab")), P(("batch", "vocab")))
    return jax.shard_map(local, mesh=mesh, in_specs=in_specs, out_specs=out_specs, check_vma=False)
```

```python
import functools

import jax
import jax.numpy as jnp
from jax import lax
from jax.experimental import pallas as pl
from jax.experimental.pallas import tpu as pltpu
from jax.sharding import PartitionSpec as P

MESH = pl.DeviceIdType.MESH
UP, DOWN, SIDE = 0, 1, 2


def each(count, body):
    if count <= 8:
        for k in range(count):
            body(k)
    else:
        lax.fori_loop(0, count, lambda k, c: (body(k), c)[1], 0)


def kernel(n, waves, x_ref, w_hbm, heat_ref, probs_ref, lse_ref, w_ref, buf, scaled, outbox, stats, lse_col,
           w_sem, own_sem, ag_send, ag_recv, st_send, st_recv, pr_send, pr_recv):
    me = lax.axis_index("vocab")
    line = n // 2
    z, y = me // 2, lax.rem(me, 2)
    seq = x_ref.shape[0]
    rows = seq // waves
    span = n * rows
    cols = w_ref.shape[1]
    tile = min(cols, 256)

    barrier = pltpu.get_barrier_semaphore()

    def greet(k):
        pl.semaphore_signal(barrier, inc=1, device_id={"vocab": lax.rem(me + k + 1, n)}, device_id_type=MESH)

    each(n - 1, greet)
    weights = pltpu.make_async_copy(w_hbm, w_ref, w_sem)
    weights.start()
    for w in range(waves):
        pltpu.make_async_copy(x_ref.at[pl.ds(w * rows, rows)], buf.at[w, me], own_sem.at[w]).start()
    for w in range(waves):
        pltpu.make_async_copy(x_ref.at[pl.ds(w * rows, rows)], buf.at[w, me], own_sem.at[w]).wait()
    pl.semaphore_wait(barrier, n - 1)

    def hop(w, block, way):
        target = {UP: lax.rem(me + 2, n), DOWN: lax.rem(me + n - 2, n), SIDE: me + 1 - 2 * y}[way]
        return pltpu.make_async_remote_copy(
            src_ref=buf.at[w, block], dst_ref=buf.at[w, block], send_sem=ag_send.at[w, block, way],
            recv_sem=ag_recv.at[w, block], device_id={"vocab": target}, device_id_type=MESH)

    def send_own(w):
        @pl.when(z < line - 1)
        def _():
            hop(w, me, UP).start()

        @pl.when(z > 0)
        def _():
            hop(w, me, DOWN).start()

        hop(w, me, SIDE).start()

    def relay(w, k):
        @pl.when(z >= k)
        def _():
            block = (z - k) * 2 + y
            hop(w, block, SIDE).wait_recv()

            @pl.when(z < line - 1)
            def _():
                hop(w, block, UP).start()

            hop(w, block, SIDE).start()

        @pl.when(z + k < line)
        def _():
            block = (z + k) * 2 + y
            hop(w, block, SIDE).wait_recv()

            @pl.when(z > 0)
            def _():
                hop(w, block, DOWN).start()

            hop(w, block, SIDE).start()

    def stat_copy(w, k):
        return pltpu.make_async_remote_copy(
            src_ref=stats.at[w, me], dst_ref=stats.at[w, me], send_sem=st_send.at[w, k],
            recv_sem=st_recv.at[w, me], device_id={"vocab": lax.rem(me + k + 1, n)}, device_id_type=MESH)

    def stat_wait(w, k):
        other = lax.rem(me + k + 1, n)
        pltpu.make_async_remote_copy(
            src_ref=stats.at[w, other], dst_ref=stats.at[w, other], send_sem=st_send.at[w, k],
            recv_sem=st_recv.at[w, other], device_id={"vocab": other}, device_id_type=MESH).wait_recv()

    def out_at(w, owner):
        return probs_ref.at[pl.ds(w * rows, rows), pl.ds(pl.multiple_of(owner * cols, cols), cols)]

    def prob_copy(w, k):
        other = lax.rem(me + k + 1, n)
        return pltpu.make_async_remote_copy(
            src_ref=outbox.at[w, other], dst_ref=out_at(w, me), send_sem=pr_send.at[w, k],
            recv_sem=pr_recv.at[w, me], device_id={"vocab": other}, device_id_type=MESH)

    def prob_wait(w, k):
        other = lax.rem(me + k + 1, n)
        pltpu.make_async_remote_copy(
            src_ref=outbox.at[w, other], dst_ref=out_at(w, other), send_sem=pr_send.at[w, k],
            recv_sem=pr_recv.at[w, other], device_id={"vocab": other}, device_id_type=MESH).wait_recv()

    def score(w):
        def arrive(k):
            hop(w, k * 2 + 1 - y, SIDE).wait_recv()

        each(line, arrive)
        if w == 0:
            weights.wait()
        hidden = buf[w].reshape(span, buf.shape[3])
        cool = 1.0 / jnp.broadcast_to(heat_ref[w], (8, span)).T[:, :1]

        def column(j, peak):
            at = pl.ds(pl.multiple_of(j * tile, tile), tile)
            logits = jnp.dot(hidden, w_ref[:, at], preferred_element_type=jnp.float32)
            s = 30.0 * jnp.tanh(logits * (1.0 / 30.0)) * cool
            scaled[:, at] = s
            return jnp.maximum(peak, jnp.max(s, axis=1, keepdims=True))

        peak = lax.fori_loop(0, cols // tile, column, jnp.full((span, 1), -jnp.inf, jnp.float32))
        total = jnp.sum(jnp.exp(scaled[...] - peak), axis=1, keepdims=True)
        lane = lax.broadcasted_iota(jnp.int32, (span, 128), 1)
        stats[w, me] = jnp.where(lane == 0, peak, total).T[:8]
        each(n - 1, lambda k: stat_copy(w, k).start())

    def finish(w):
        each(n - 1, lambda k: stat_wait(w, k))
        got = stats[w]
        peaks, totals = got[:, 0, :], got[:, 1, :]
        peak = jnp.max(peaks, axis=0, keepdims=True)
        lse = peak + jnp.log(jnp.sum(totals * jnp.exp(peaks - peak), axis=0, keepdims=True))
        lse = jnp.broadcast_to(lse, (8, span)).T[:, :1]
        probs = jnp.exp(scaled[...] - lse).astype(jnp.bfloat16)
        outbox[w] = probs.reshape(n, rows, cols)
        each(n - 1, lambda k: prob_copy(w, k).start())
        lse_col[...] = jnp.broadcast_to(lse, (span, 128)).reshape(n, rows, 128)
        lse_ref[pl.ds(w * rows, rows), :] = lse_col[me]
        probs_ref[pl.ds(w * rows, rows), pl.ds(pl.multiple_of(me * cols, cols), cols)] = outbox[w, me]

    send_own(0)
    for w in range(waves):
        todo = []
        if w >= 1:
            todo = [functools.partial(score, w - 1), functools.partial(finish, w - 1)]
        if line - 1 <= 8:
            if w + 1 < waves:
                send_own(w + 1)
            for k in range(1, line):
                relay(w, k)
                if todo:
                    todo.pop(0)()
        else:
            if w + 1 < waves:
                send_own(w + 1)
            each(line - 1, lambda k: relay(w, k + 1))
        while todo:
            todo.pop(0)()
    score(waves - 1)
    finish(waves - 1)

    for w in range(waves):
        each(n - 1, lambda k: prob_wait(w, k))

        def drain(k):
            block = k * 2 + y

            @pl.when(jnp.logical_and(z < line - 1, k <= z))
            def _():
                hop(w, block, UP).wait_send()

            @pl.when(jnp.logical_and(z > 0, k >= z))
            def _():
                hop(w, block, DOWN).wait_send()

            hop(w, block, SIDE).wait_send()

        each(line, drain)
        each(n - 1, lambda k: stat_copy(w, k).wait_send())
        each(n - 1, lambda k: prob_copy(w, k).wait_send())


def solution(mesh):
    n = mesh.shape["vocab"]

    def local(latent_vectors, unembedding_matrix, sampler_heat):
        seq, depth = latent_vectors.shape
        cols = unembedding_matrix.shape[1]
        waves = max(1, seq // 32)
        rows = seq // waves
        span = n * rows
        heat = sampler_heat.reshape(n, waves, rows).transpose(1, 0, 2).reshape(waves, 1, span)
        vmem = pl.BlockSpec(memory_space=pltpu.VMEM)
        dma = pltpu.SemaphoreType.DMA
        probs, lse = pl.pallas_call(
            functools.partial(kernel, n, waves),
            out_shape=(jax.ShapeDtypeStruct((seq, n * cols), jnp.bfloat16),
                       jax.ShapeDtypeStruct((seq, 128), jnp.float32)),
            in_specs=[vmem, pl.BlockSpec(memory_space=pl.ANY), vmem],
            out_specs=(vmem, vmem),
            scratch_shapes=[
                pltpu.VMEM((depth, cols), jnp.bfloat16),
                pltpu.VMEM((waves, n, rows, depth), jnp.bfloat16),
                pltpu.VMEM((span, cols), jnp.float32),
                pltpu.VMEM((waves, n, rows, cols), jnp.bfloat16),
                pltpu.VMEM((waves, n, 8, span), jnp.float32),
                pltpu.VMEM((n, rows, 128), jnp.float32),
                dma, dma((waves,)),
                dma((waves, n, 3)), dma((waves, n)),
                dma((waves, n - 1)), dma((waves, n)),
                dma((waves, n - 1)), dma((waves, n)),
            ],
            compiler_params=pltpu.CompilerParams(
                collective_id=0, has_side_effects=True, vmem_limit_bytes=56 * 1024 * 1024),
        )(latent_vectors, unembedding_matrix, heat)
        lse = lse[:, 0]
        return probs, lse, 0.0001 * lse * lse

    in_specs = (P(("batch", "vocab"), None), P("batch", "vocab"), P("batch"))
    out_specs = (P(("batch", "vocab"), None), P(("batch", "vocab")), P(("batch", "vocab")))
    return jax.shard_map(local, mesh=mesh, in_specs=in_specs, out_specs=out_specs, check_vma=False)
```
